32 devices in a mesh: snap: 8 (over z, y), row: 4 (over x, core).
Axes of the slice: x: 2, y: 2, z: 4, core: 2. Of those that a mesh axis runs over, the one named last changes fastest.
Arguments:
- snapshots: bfloat16 [48, 256, 8192], P('snap', 'row'), may hold values from -6 to 6
- counts: int32 [8], P('snap'), may hold values from 1 to 6, 32 in all
- order: int32 [32], P(('snap', 'row')), may hold values from 0 to 31, each once
- coefficients: float32 [3, 32], replicated, may hold values from -1 to 1
Outputs:
- widths: bfloat16 [3, 256, 8192], P(None, 'row', 'snap')
The draws below stay inside these ranges and needn't reach their ends.
Inputs may be any that keep to these rules, and one draw needn't show every extreme that they name: Holder d's live snapshots are its first counts[d] slots; counts sum to 32, and some holder stores 6.
All inputs are finite; a program needn't handle non-finite values. No bound on the sum of `counts` on one device may be relied on, other than what follows from the above.
Results may differ from the reference program's by a relative error of at most 0.001.
Values may be sent and summed in bfloat16 or wider, within the bound.
No kernel may reach another device: no remote copies, remote signals or barrier semaphores. Data moves between devices by JAX's collectives and lax.ppermute only.
A program may use at most 64 MiB of HBM per device.

```python
import math
import jax
import jax.numpy as jnp
import numpy as np
from jax import lax

D = 8192
MAXS = 6
K = 3
ROWS = 256
SLOTS = 48
TOTAL = 32
N_SNAP = 8


def with_spikes(result, own_key, source, target, shards_of, factor):
    owner, partner = [(jnp.arange(result.shape[axis_at]) // (result.shape[axis_at] // shards_of)).reshape([-1 if axis == axis_at else 1 for axis in range(result.ndim)]) for axis_at in (source, target)]
    chosen = jax.random.permutation(own_key, shards_of)[partner]
    strong = (owner == chosen) | (owner == (partner + shards_of // 2) % shards_of)
    return jnp.where(strong, factor * result, result)


def level_of(rng, dims, shards, low, top_value):
    gain, own = 1.0, jax.random.fold_in(rng, 6)
    for dim, parts in shards:
        draws = jnp.exp(jax.random.uniform(jax.random.fold_in(own, dim), (parts,), jnp.float32, low / len(shards), top_value / len(shards)))
        gain = gain * jnp.repeat(draws, dims[dim] // parts).reshape([-1 if axis == dim else 1 for axis in range(len(dims))])
    return gain


def split_up(amount, total, most, slope):
    loads = [(1 << 20) // math.isqrt(standing ** slope) + 1 for standing in range(2, amount + 1)]
    surplus, holding = total - most - (amount - 1), [1] * (amount - 1)
    while surplus > 0:
        movable = [i for i in range(amount - 1) if holding[i] < most]
        mass, budget = sum([loads[i] for i in movable]), surplus
        for i in movable:
            addition = min(most - holding[i], max(1, budget * loads[i] // mass), surplus)
            holding[i] = holding[i] + addition
            surplus = surplus - addition
    return np.array([most] + holding)


def ragged_sizes(key, count, total, reach, skew):
    if count == 2:
        one = jax.random.randint(key, (), max(1, total - reach), min(reach, total - 1) + 1)
        return jnp.stack([one, total - one])
    lengths = jnp.asarray(split_up(count, total, reach, skew), jnp.int32)
    twos = (count - 1) // 2
    giver, taker = lengths[1:1 + 2 * twos:2], lengths[2:2 + 2 * twos:2]
    slack = jnp.minimum(giver - 1, reach - taker)
    shifted = jax.random.randint(jax.random.fold_in(key, 1), (twos,), 0, 1 << 20) % (slack + 1)
    lengths = lengths.at[1:1 + 2 * twos:2].set(giver - shifted).at[2:2 + 2 * twos:2].set(taker + shifted)
    return lengths[jax.random.permutation(jax.random.fold_in(key, 2), count)]


def noise(stream_key, extent, deviation, bound, shards=(), kind=jnp.bfloat16):
    loudness = level_of(stream_key, extent, shards, -0.22, 0.18) if shards else 1.0
    entries = jax.random.normal(stream_key, extent, jnp.float32) * deviation * loudness
    return jnp.minimum(jnp.maximum(entries, -bound), bound).astype(kind)


def bell_draw_with(stream_key, shape, spread, most, cuts, heavy, kind=jnp.bfloat16):
    result = spread * jax.random.normal(stream_key, shape, jnp.float32)
    if cuts:
        result = result * level_of(stream_key, shape, cuts, -0.22, 0.18)
    return jnp.clip(with_spikes(result, jax.random.fold_in(stream_key, 3), *heavy), -most, most).astype(kind)


def setup_inputs(seed: int = 0) -> dict:
    key_of = jax.random.split(jax.random.key(seed), 5)
    return {
        "snapshots": bell_draw_with(key_of[0], (SLOTS, ROWS, D), 1.0, 6.0, ((0, 8), (1, 4)), (0, 2, 8, 2.0)),
        "counts": ragged_sizes(key_of[1], N_SNAP, TOTAL, MAXS, 2).astype(jnp.int32),
        "order": jax.random.permutation(key_of[2], TOTAL).astype(jnp.int32),
        "coefficients": noise(key_of[3], (K, TOTAL), TOTAL ** -0.5, 1.0, (), jnp.float32),
    }


def reference(snapshots, counts, order, coefficients):
    starts = jnp.cumsum(counts).astype(jnp.int32) - counts
    slot_index = jnp.arange(SLOTS, dtype=jnp.int32)
    holder = slot_index // MAXS
    within = slot_index % MAXS
    is_live = within < counts[holder]
    position = ((starts[holder] + within + TOTAL // 2) % TOTAL).astype(jnp.int32)
    ident = order[position]
    weights = jnp.where(is_live[None, :], coefficients[:, ident], jnp.float32(0.0)).astype(jnp.float32)

    def add_slot(running, pair):
        column, snapshot = pair
        return running + column[:, None, None] * snapshot.astype(jnp.float32)[None], None

    start_sum = jnp.zeros((K, ROWS, D), jnp.float32)
    running, _ = lax.scan(add_slot, start_sum, (weights.T, snapshots))
    return running.astype(jnp.bfloat16)
```

```python
import functools

import jax
import jax.numpy as jnp
from jax import lax
from jax.experimental import pallas as pl
from jax.experimental.pallas import tpu as pltpu
from jax.sharding import PartitionSpec as P


LANES = 128
TALL = 16
VMEM_LIMIT = 24 * 1024 * 1024
TOP = 32600.0
STEPS = 64.0
LN2 = 0.6931471805599453
COUNT_BITS = 10
COUNT_MASK = (1 << COUNT_BITS) - 1


def weights_of(holder, group, table_ref, coef_ref, slots):
    total = table_ref.shape[0]
    start = lax.fori_loop(
        0,
        holder,
        lambda e, s: s + (table_ref[e * group, 0] & COUNT_MASK),
        jnp.int32(0),
    )
    count = table_ref[holder * group, 0] & COUNT_MASK
    weights = [[] for _ in range(coef_ref.shape[0])]
    for j in range(slots):
        position = start + j + total // 2
        position = jnp.where(position >= total, position - total, position)
        ident = table_ref[position, 0] >> COUNT_BITS
        for k, row in enumerate(weights):
            row.append(jnp.where(j < count, coef_ref[k, ident], 0.0))
    return weights


def tile_sums(sources, received, tiles, tile):
    kinds = len(sources[0][0])
    accs = [None] * kinds
    for w, x_ref, rows, cols in sources:
        for j in range(x_ref.shape[0]):
            own = x_ref[j, rows, cols].astype(jnp.float32)
            for k in range(kinds):
                term = w[k][j] * own
                accs[k] = term if accs[k] is None else accs[k] + term
    for block, scales in received:
        for k in range(kinds):
            at = (k * tiles + tile) * TALL
            code = block[pl.ds(at, TALL), :].astype(jnp.int32).astype(jnp.float32)
            accs[k] = accs[k] + code * scales[k]
    return accs


def scales_of(block, tiles, kinds):
    code = block[pl.ds(kinds * tiles * TALL, TALL), :].astype(jnp.int32)
    scale = jnp.exp(code.astype(jnp.float32) * (LN2 / STEPS))
    return [scale[k : k + 1, :] for k in range(kinds)]


def tiles_of(height, width):
    return [(r, c) for r in range(0, height, TALL) for c in range(0, width, LANES)]


def patterns_of(stage, bits):
    depth = min(2, bits - 1 - stage)
    found = [()]
    for _ in range(depth):
        found = [p + (v,) for p in found for v in (1, 0)]
    return found


def piece_size(stage, bits):
    return 1 << max(0, bits - 3 - stage)


def mask_of(stage, pattern, r, order):
    mask = 1 << order[stage]
    for v, b in zip(pattern, order[stage + 1 :]):
        mask = mask | (v << b)
    for place, b in enumerate(reversed(order[stage + 1 + len(pattern) :])):
        mask = mask | (((r >> place) & 1) << b)
    return mask


def source_of(earlier, stage, pattern, bits):
    known = (0,) * (stage - earlier - 1) + ((1,) if stage < bits else ()) + pattern
    depth = min(2, bits - 1 - earlier)
    known = known[: bits - 1 - earlier]
    free = bits - 1 - earlier - len(known)
    first = 0
    for v in known[depth:]:
        first = first * 2 + v
    return known[:depth], first << free


def send_kernel(
    group, flows, stage, launch, plan, kinds, me_ref, table_ref, coef_ref, x_ref, *refs
):
    bits = len(flows[0][2])
    count = len(flows) * len(launch)
    *inputs, sum_ref = refs
    inputs, outputs = inputs[:-count], inputs[-count:]
    me = me_ref[0]
    slots = x_ref.shape[0]
    width = x_ref.shape[2] >> bits
    size = piece_size(stage, bits)

    w = weights_of(me, group, table_ref, coef_ref, slots)
    for p, pattern in enumerate(launch):
        for f, (first, height, order) in enumerate(flows):
            tiles = tiles_of(height, width)
            out_ref = outputs[f * len(launch) + p]

            def one(r, carry):
                dest = me ^ mask_of(stage, pattern, r, order)
                blocks = [inputs[at * len(flows) + f].at[base + r] for at, base in plan[p]]
                received = [(b, scales_of(b, len(tiles), kinds)) for b in blocks]
                peaks = [jnp.zeros((8, LANES), jnp.float32)] * kinds
                for t, (row, c) in enumerate(tiles):
                    cols = pl.ds(pl.multiple_of(dest * width + c, LANES), LANES)
                    sources = [(w, x_ref, pl.ds(first + row, TALL), cols)]
                    accs = tile_sums(sources, received, len(tiles), t)
                    for k in range(kinds):
                        sum_ref[pl.ds((k * len(tiles) + t) * TALL, TALL), :] = accs[k]
                        amount = jnp.abs(accs[k])
                        peaks[k] = jnp.maximum(
                            peaks[k], jnp.maximum(amount[:8], amount[8:])
                        )
                row_index = lax.broadcasted_iota(jnp.int32, (TALL, LANES), 0)
                codes = jnp.zeros((TALL, LANES), jnp.int32)
                for k in range(kinds):
                    peak = jnp.max(peaks[k], axis=0, keepdims=True)
                    step = jnp.ceil(
                        jnp.log(jnp.maximum(peak, 1e-30) * (1.0 / TOP)) * (STEPS / LN2)
                    )
                    gain = jnp.exp(step * (-LN2 / STEPS))
                    codes = jnp.where(row_index == k, step.astype(jnp.int32), codes)
                    for t in range(len(tiles)):
                        at = pl.ds((k * len(tiles) + t) * TALL, TALL)
                        code = jnp.round(sum_ref[at, :] * gain)
                        out_ref[r, at, :] = code.astype(jnp.int32).astype(jnp.int16)
                out_ref[r, pl.ds(kinds * len(tiles) * TALL, TALL), :] = codes.astype(jnp.int16)
                return carry

            lax.fori_loop(0, size, one, 0)


def held_kernel(group, flows, plan, kinds, me_ref, table_ref, coef_ref, x_ref, *refs):
    bits = len(flows[0][2])
    *inputs, held_ref = refs
    me = me_ref[0]
    w = weights_of(me, group, table_ref, coef_ref, x_ref.shape[0])
    width = x_ref.shape[2] >> bits
    for f, (first, height, _) in enumerate(flows):
        tiles = tiles_of(height, width)
        blocks = [inputs[at * len(flows) + f].at[base] for at, base in plan[0]]
        received = [(b, scales_of(b, len(tiles), kinds)) for b in blocks]
        for t, (row, c) in enumerate(tiles):
            rows = pl.ds(first + row, TALL)
            cols = pl.ds(pl.multiple_of(me * width + c, LANES), LANES)
            accs = tile_sums([(w, x_ref, rows, cols)], received, len(tiles), t)
            for k in range(kinds):
                held_ref[k, rows, c : c + LANES] = accs[k]


def last_kernel(flows, kinds, held_ref, *refs):
    *inputs, out_ref = refs
    width = held_ref.shape[2]
    for (first, height, _), ref in zip(flows, inputs):
        tiles = tiles_of(height, width)
        block = ref.at[0]
        scales = scales_of(block, len(tiles), kinds)
        for t, (row, c) in enumerate(tiles):
            for k in range(kinds):
                at = (pl.ds(first + row, TALL), slice(c, c + LANES))
                code = block[pl.ds((k * len(tiles) + t) * TALL, TALL), :]
                code = code.astype(jnp.int32).astype(jnp.float32)
                total = held_ref[(k, *at)] + code * scales[k]
                out_ref[(k, *at)] = total.astype(jnp.bfloat16)


def block_rows(flow, kinds, width):
    return kinds * len(tiles_of(flow[1], width)) * TALL + TALL


SMEM = pl.BlockSpec(memory_space=pltpu.SMEM)
VMEM = pl.BlockSpec(memory_space=pltpu.VMEM)
PARAMS = pltpu.CompilerParams(vmem_limit_bytes=VMEM_LIMIT)


def cost(elements, slots):
    return pl.CostEstimate(
        flops=2 * slots * elements, bytes_accessed=8 * elements, transcendentals=0
    )


def gather_plan(chosen, bits, stage, launch, arrived, until):
    keys, plan = [], []
    for pattern in launch:
        sources = []
        for earlier in range(until):
            found, base = source_of(earlier, stage, pattern, bits)
            if (earlier, found) not in keys:
                keys.append((earlier, found))
            sources.append((keys.index((earlier, found)), base))
        plan.append(sources)
    return [arrived[(*key, f)] for key in keys for f in chosen], plan


def send_call(flows, chosen, stage, launch, group, me, table, coef, x, arrived):
    bits = len(flows[0][2])
    kinds = coef.shape[0]
    width = x.shape[2] >> bits
    arrays, plan = gather_plan(chosen, bits, stage, launch, arrived, stage)
    mine = [flows[f] for f in chosen]
    shapes = [
        jax.ShapeDtypeStruct(
            (piece_size(stage, bits), block_rows(flow, kinds, width), LANES), jnp.int16
        )
        for flow in mine
        for _ in launch
    ]
    tallest = max(block_rows(flow, kinds, width) for flow in mine)
    height = sum(flow[1] for flow in mine)
    blocks = piece_size(stage, bits) * len(launch)
    sent = pl.pallas_call(
        functools.partial(send_kernel, group, mine, stage, launch, plan, kinds),
        in_specs=[SMEM, SMEM, SMEM, VMEM] + [VMEM] * len(arrays),
        out_specs=[VMEM] * len(shapes),
        out_shape=shapes,
        scratch_shapes=[pltpu.VMEM((tallest, LANES), jnp.float32)],
        compiler_params=PARAMS,
        cost_estimate=cost(kinds * height * width * blocks, x.shape[0]),
    )(me, table, coef, x, *arrays)
    return {
        (p, f): sent[at * len(launch) + i]
        for at, f in enumerate(chosen)
        for i, p in enumerate(launch)
    }


def last_calls(flows, group, me, table, coef, x, arrived):
    bits = len(flows[0][2])
    kinds = coef.shape[0]
    width = x.shape[2] >> bits
    chosen = tuple(range(len(flows)))
    arrays, plan = gather_plan(chosen, bits, bits, [()], arrived, bits - 1)
    shape = (kinds, x.shape[1], width)
    elements = kinds * x.shape[1] * width
    held = pl.pallas_call(
        functools.partial(held_kernel, group, flows, plan, kinds),
        in_specs=[SMEM, SMEM, SMEM, VMEM] + [VMEM] * len(arrays),
        out_specs=VMEM,
        out_shape=jax.ShapeDtypeStruct(shape, jnp.float32),
        compiler_params=PARAMS,
        cost_estimate=cost(elements, x.shape[0]),
    )(me, table, coef, x, *arrays)
    return pl.pallas_call(
        functools.partial(last_kernel, flows, kinds),
        in_specs=[VMEM] * (1 + len(flows)),
        out_specs=VMEM,
        out_shape=jax.ShapeDtypeStruct(shape, jnp.bfloat16),
        compiler_params=PARAMS,
        cost_estimate=cost(elements, 2),
    )(held, *[arrived[bits - 1, (), f] for f in chosen])


def schedule_of(bits):
    make, move = (lambda *a: ("make", a)), (lambda *a: ("move", a))
    if bits == 3:
        steps = []
        for stage, pattern, f in (
            (0, (1, 1), 0),
            (0, (1, 1), 1),
            (0, (0, 1), 0),
            (1, (1,), 0),
            (0, (0, 1), 1),
            (1, (1,), 1),
        ):
            steps += [make(stage, (pattern,), (f,)), move(stage, pattern, f)]
        return steps + [
            make(0, ((1, 0), (0, 0)), (0, 1)),
            make(2, ((),), (0,)),
            move(2, (), 0),
            move(0, (1, 0), 0),
            move(0, (1, 0), 1),
            make(2, ((),), (1,)),
            move(2, (), 1),
            move(0, (0, 0), 0),
            move(0, (0, 0), 1),
            make(1, ((0,),), (0, 1)),
            move(1, (0,), 0),
            move(1, (0,), 1),
        ]
    steps = []
    for stage in range(bits):
        for pattern in patterns_of(stage, bits):
            steps.append(make(stage, (pattern,), (0, 1)))
            steps += [move(stage, pattern, f) for f in (0, 1)]
    return steps


def on_device(snapshots, counts, order, coefficients):
    owners, group = lax.axis_size("snap"), lax.axis_size("row")
    bits = owners.bit_length() - 1
    half = snapshots.shape[1] // 2
    swapped = tuple([1, 0] + list(range(2, bits)))
    flows = ((0, half, tuple(range(bits))), (half, half, swapped))
    me = lax.axis_index("snap").reshape(1)
    own = (order << COUNT_BITS) + counts
    table = lax.all_to_all(
        jnp.broadcast_to(own[:, None], (owners * group, 1)), ("snap", "row"), 0, 0, tiled=True
    )
    made, arrived = {}, {}
    for kind, step in schedule_of(bits):
        if kind == "make":
            stage, launch, chosen = step
            sent = send_call(
                flows, chosen, stage, launch, group, me, table, coefficients,
                snapshots, arrived,
            )
            made.update({(stage, *key): value for key, value in sent.items()})
        else:
            stage, _, f = step
            pairs = [(d, d ^ (1 << flows[f][2][stage])) for d in range(owners)]
            arrived[step] = lax.ppermute(made[step], "snap", pairs)
    return last_calls(flows, group, me, table, coefficients, snapshots, arrived)


def solution(mesh):
    return jax.shard_map(
        on_device,
        mesh=mesh,
        in_specs=(P("snap", "row", None), P("snap"), P(("snap", "row")), P()),
        out_specs=P(None, "row", "snap"),
        check_vma=False,
    )
```

```python
import functools

import jax
import jax.numpy as jnp
from jax import lax
from jax.experimental import pallas as pl
from jax.experimental.pallas import tpu as pltpu
from jax.sharding import PartitionSpec as P


LANES = 128
TALL = 16
VMEM_LIMIT = 24 * 1024 * 1024
PACK_LIMIT = 58 * 1024 * 1024
TOP = 32600.0
STEPS = 64.0
LN2 = 0.6931471805599453
COUNT_BITS = 10
COUNT_MASK = (1 << COUNT_BITS) - 1


def weights_of(holder, group, table_ref, coef_ref, slots):
    total = table_ref.shape[0]
    start = lax.fori_loop(
        0,
        holder,
        lambda e, s: s + (table_ref[e * group, 0] & COUNT_MASK),
        jnp.int32(0),
    )
    count = table_ref[holder * group, 0] & COUNT_MASK
    weights = [[] for _ in range(coef_ref.shape[0])]
    for j in range(slots):
        position = start + j + total // 2
        position = jnp.where(position >= total, position - total, position)
        ident = table_ref[position, 0] >> COUNT_BITS
        for k, row in enumerate(weights):
            row.append(jnp.where(j < count, coef_ref[k, ident], 0.0))
    return weights


def tile_sums(sources, received, tiles, tile):
    kinds = len(sources[0][0])
    accs = [None] * kinds
    for w, x_ref, rows, cols in sources:
        for j in range(x_ref.shape[0]):
            own = x_ref[j, rows, cols].astype(jnp.float32)
            for k in range(kinds):
                term = w[k][j] * own
                accs[k] = term if accs[k] is None else accs[k] + term
    for block, scales in received:
        for k in range(kinds):
            at = (k * tiles + tile) * TALL
            code = block[pl.ds(at, TALL), :].astype(jnp.int32).astype(jnp.float32)
            accs[k] = accs[k] + code * scales[k]
    return accs


def scales_of(block, tiles, kinds):
    code = block[pl.ds(kinds * tiles * TALL, TALL), :].astype(jnp.int32)
    scale = jnp.exp(code.astype(jnp.float32) * (LN2 / STEPS))
    return [scale[k : k + 1, :] for k in range(kinds)]


def tiles_of(height, width):
    return [(r, c) for r in range(0, height, TALL) for c in range(0, width, LANES)]


def patterns_of(stage, bits):
    depth = min(2, bits - 1 - stage)
    found = [()]
    for _ in range(depth):
        found = [p + (v,) for p in found for v in (1, 0)]
    return found


def piece_size(stage, bits):
    return 1 << max(0, bits - 3 - stage)


def mask_of(stage, pattern, r, order):
    mask = 1 << order[stage]
    for v, b in zip(pattern, order[stage + 1 :]):
        mask = mask | (v << b)
    for place, b in enumerate(reversed(order[stage + 1 + len(pattern) :])):
        mask = mask | (((r >> place) & 1) << b)
    return mask


def source_of(earlier, stage, pattern, bits):
    known = (0,) * (stage - earlier - 1) + ((1,) if stage < bits else ()) + pattern
    depth = min(2, bits - 1 - earlier)
    known = known[: bits - 1 - earlier]
    free = bits - 1 - earlier - len(known)
    first = 0
    for v in known[depth:]:
        first = first * 2 + v
    return known[:depth], first << free


def send_kernel(
    group, flows, stage, launch, plan, kinds, me_ref, table_ref, coef_ref, x_ref, *refs
):
    bits = len(flows[0][2])
    count = len(flows) * len(launch)
    *inputs, sum_ref = refs
    inputs, outputs = inputs[:-count], inputs[-count:]
    me = me_ref[0]
    slots = x_ref.shape[0]
    width = x_ref.shape[2] >> bits
    size = piece_size(stage, bits)

    w = weights_of(me, group, table_ref, coef_ref, slots)
    for p, pattern in enumerate(launch):
        for f, (first, height, order) in enumerate(flows):
            tiles = tiles_of(height, width)
            out_ref = outputs[f * len(launch) + p]

            def one(r, carry):
                dest = me ^ mask_of(stage, pattern, r, order)
                blocks = [inputs[at * len(flows) + f].at[base + r] for at, base in plan[p]]
                received = [(b, scales_of(b, len(tiles), kinds)) for b in blocks]
                peaks = [jnp.zeros((8, LANES), jnp.float32)] * kinds
                for t, (row, c) in enumerate(tiles):
                    cols = pl.ds(pl.multiple_of(dest * width + c, LANES), LANES)
                    sources = [(w, x_ref, pl.ds(first + row, TALL), cols)]
                    accs = tile_sums(sources, received, len(tiles), t)
                    for k in range(kinds):
                        sum_ref[pl.ds((k * len(tiles) + t) * TALL, TALL), :] = accs[k]
                        amount = jnp.abs(accs[k])
                        peaks[k] = jnp.maximum(
                            peaks[k], jnp.maximum(amount[:8], amount[8:])
                        )
                row_index = lax.broadcasted_iota(jnp.int32, (TALL, LANES), 0)
                codes = jnp.zeros((TALL, LANES), jnp.int32)
                for k in range(kinds):
                    peak = jnp.max(peaks[k], axis=0, keepdims=True)
                    step = jnp.ceil(
                        jnp.log(jnp.maximum(peak, 1e-30) * (1.0 / TOP)) * (STEPS / LN2)
                    )
                    gain = jnp.exp(step * (-LN2 / STEPS))
                    codes = jnp.where(row_index == k, step.astype(jnp.int32), codes)
                    for t in range(len(tiles)):
                        at = pl.ds((k * len(tiles) + t) * TALL, TALL)
                        code = jnp.round(sum_ref[at, :] * gain)
                        out_ref[r, at, :] = code.astype(jnp.int32).astype(jnp.int16)
                out_ref[r, pl.ds(kinds * len(tiles) * TALL, TALL), :] = codes.astype(jnp.int16)
                return carry

            lax.fori_loop(0, size, one, 0)


def pack_kernel(flow, me_ref, x_ref, out_ref, sem):
    first, height, order = flow
    width = x_ref.shape[2] >> len(order)
    dest = me_ref[0] ^ (1 << order[0])
    cols = pl.ds(pl.multiple_of(dest * width, LANES), width)
    copy = pltpu.make_async_copy(x_ref.at[:, pl.ds(first, height), cols], out_ref.at[0], sem)
    copy.start()
    copy.wait()


def held_kernel(group, flow, base, kinds, me_ref, table_ref, coef_ref, x_ref, piece_ref, held_ref):
    first, height, order = flow
    me = me_ref[0]
    w = weights_of(me, group, table_ref, coef_ref, x_ref.shape[0])
    width = x_ref.shape[2] >> len(order)
    tiles = tiles_of(height, width)
    block = piece_ref.at[base]
    raw = len(block.shape) == 3
    if raw:
        other = weights_of(me ^ (1 << order[0]), group, table_ref, coef_ref, x_ref.shape[0])
        received = []
    else:
        received = [(block, scales_of(block, len(tiles), kinds))]
    for t, (row, c) in enumerate(tiles):
        rows, place = pl.ds(row, TALL), pl.ds(c, LANES)
        cols = pl.ds(pl.multiple_of(me * width + c, LANES), LANES)
        sources = [(w, x_ref, pl.ds(first + row, TALL), cols)]
        if raw:
            sources.append((other, block, rows, place))
        accs = tile_sums(sources, received, len(tiles), t)
        for k in range(kinds):
            held_ref[k, rows, place] = accs[k]


def last_kernel(flows, kinds, *refs):
    *inputs, out_ref = refs
    helds, inputs = inputs[: len(flows)], inputs[len(flows) :]
    width = out_ref.shape[2]
    for f, (first, height, _) in enumerate(flows):
        held_ref = helds[f]
        tiles = tiles_of(height, width)
        blocks = [ref.at[0] for ref in inputs[f :: len(flows)]]
        scales = [scales_of(block, len(tiles), kinds) for block in blocks]
        for t, (row, c) in enumerate(tiles):
            for k in range(kinds):
                total = held_ref[k, row : row + TALL, c : c + LANES]
                for block, scale in zip(blocks, scales):
                    code = block[pl.ds((k * len(tiles) + t) * TALL, TALL), :]
                    total = total + code.astype(jnp.int32).astype(jnp.float32) * scale[k]
                rows = slice(first + row, first + row + TALL)
                out_ref[k, rows, c : c + LANES] = total.astype(jnp.bfloat16)


def block_rows(flow, kinds, width):
    return kinds * len(tiles_of(flow[1], width)) * TALL + TALL


SMEM = pl.BlockSpec(memory_space=pltpu.SMEM)
VMEM = pl.BlockSpec(memory_space=pltpu.VMEM)
ANY = pl.BlockSpec(memory_space=pl.ANY)
PARAMS = pltpu.CompilerParams(vmem_limit_bytes=VMEM_LIMIT)


def cost(elements, slots):
    return pl.CostEstimate(
        flops=2 * slots * elements, bytes_accessed=8 * elements, transcendentals=0
    )


def pack_call(flow, me, x):
    width = x.shape[2] >> len(flow[2])
    shape = (1, x.shape[0], flow[1], width)
    return pl.pallas_call(
        functools.partial(pack_kernel, flow),
        in_specs=[SMEM, ANY],
        out_specs=VMEM,
        out_shape=jax.ShapeDtypeStruct(shape, x.dtype),
        scratch_shapes=[pltpu.SemaphoreType.DMA],
        compiler_params=pltpu.CompilerParams(vmem_limit_bytes=PACK_LIMIT),
        cost_estimate=cost(x.size >> 4, 1),
    )(me, x)


def gather_plan(chosen, bits, stage, launch, arrived, until):
    keys, plan = [], []
    for pattern in launch:
        sources = []
        for earlier in range(until):
            found, base = source_of(earlier, stage, pattern, bits)
            if (earlier, found) not in keys:
                keys.append((earlier, found))
            sources.append((keys.index((earlier, found)), base))
        plan.append(sources)
    return [arrived[(*key, f)] for key in keys for f in chosen], plan


def send_call(flows, chosen, stage, launch, group, me, table, coef, x, arrived):
    bits = len(flows[0][2])
    kinds = coef.shape[0]
    width = x.shape[2] >> bits
    arrays, plan = gather_plan(chosen, bits, stage, launch, arrived, stage)
    mine = [flows[f] for f in chosen]
    shapes = [
        jax.ShapeDtypeStruct(
            (piece_size(stage, bits), block_rows(flow, kinds, width), LANES), jnp.int16
        )
        for flow in mine
        for _ in launch
    ]
    tallest = max(block_rows(flow, kinds, width) for flow in mine)
    height = sum(flow[1] for flow in mine)
    blocks = piece_size(stage, bits) * len(launch)
    sent = pl.pallas_call(
        functools.partial(send_kernel, group, mine, stage, launch, plan, kinds),
        in_specs=[SMEM, SMEM, SMEM, VMEM] + [VMEM] * len(arrays),
        out_specs=[VMEM] * len(shapes),
        out_shape=shapes,
        scratch_shapes=[pltpu.VMEM((tallest, LANES), jnp.float32)],
        compiler_params=PARAMS,
        cost_estimate=cost(kinds * height * width * blocks, x.shape[0]),
    )(me, table, coef, x, *arrays)
    return {
        (p, f): sent[at * len(launch) + i]
        for at, f in enumerate(chosen)
        for i, p in enumerate(launch)
    }


def held_call(flow, f, group, me, table, coef, x, arrived):
    bits = len(flow[2])
    kinds = coef.shape[0]
    width = x.shape[2] >> bits
    found, base = source_of(0, bits, (), bits)
    return pl.pallas_call(
        functools.partial(held_kernel, group, flow, base, kinds),
        in_specs=[SMEM, SMEM, SMEM, VMEM, VMEM],
        out_specs=VMEM,
        out_shape=jax.ShapeDtypeStruct((kinds, flow[1], width), jnp.float32),
        compiler_params=PARAMS,
        cost_estimate=cost(kinds * flow[1] * width, x.shape[0]),
    )(me, table, coef, x, arrived[0, found, f])


def last_call(flows, x, helds, arrived):
    bits = len(flows[0][2])
    kinds = helds[0].shape[0]
    shape = (kinds, x.shape[1], x.shape[2] >> bits)
    arrays = [
        arrived[earlier, source_of(earlier, bits, (), bits)[0], f]
        for earlier in range(1, bits)
        for f in range(len(flows))
    ]
    return pl.pallas_call(
        functools.partial(last_kernel, flows, kinds),
        in_specs=[VMEM] * (len(flows) + len(arrays)),
        out_specs=VMEM,
        out_shape=jax.ShapeDtypeStruct(shape, jnp.bfloat16),
        compiler_params=PARAMS,
        cost_estimate=cost(kinds * x.shape[1] * shape[2], 2),
    )(*helds, *arrays)


def schedule_of(bits):
    make, move = (lambda *a: ("make", a)), (lambda *a: ("move", a))
    hold = lambda f: ("hold", f)
    if bits == 3:
        return [
            make(0, ((1, 1),), (0, 1)),
            move(0, (1, 1), 0),
            move(0, (1, 1), 1),
            make(0, ((0, 1),), (0,)),
            move(0, (0, 1), 0),
            make(0, ((0, 1),), (1,)),
            make(1, ((1,),), (0,)),
            move(1, (1,), 0),
            move(0, (0, 1), 1),
            make(1, ((1,),), (1,)),
            move(1, (1,), 1),
            make(0, ((1, 0), (0, 0)), (0,)),
            move(0, (1, 0), 0),
            make(2, ((),), (0,)),
            move(2, (), 0),
            make(0, ((1, 0),), (1,)),
            move(0, (1, 0), 1),
            move(0, (0, 0), 0),
            make(2, ((),), (1,)),
            move(2, (), 1),
            hold(1),
            make(1, ((0,),), (0,)),
            move(1, (0,), 0),
            make(1, ((0,),), (1,)),
            move(1, (0,), 1),
            hold(0),
        ]
    steps = []
    for stage in range(bits):
        for pattern in patterns_of(stage, bits):
            steps.append(make(stage, (pattern,), (0, 1)))
            steps += [move(stage, pattern, f) for f in (0, 1)]
    return steps + [hold(0), hold(1)]


def on_device(snapshots, counts, order, coefficients):
    owners, group = lax.axis_size("snap"), lax.axis_size("row")
    bits = owners.bit_length() - 1
    half = snapshots.shape[1] // 2
    swapped = tuple([1, 0] + list(range(2, bits)))
    flows = ((0, half, tuple(range(bits))), (half, half, swapped))
    me = lax.axis_index("snap").reshape(1)
    own = (order << COUNT_BITS) + counts
    table = lax.all_to_all(
        jnp.broadcast_to(own[:, None], (owners * group, 1)),
        ("snap", "row"),
        0,
        0,
        tiled=True,
    )
    made, arrived, helds = {}, {}, {}
    if bits == 3:
        raw = pack_call(flows[1], me, snapshots)
        pairs = [(d, d ^ (1 << flows[1][2][0])) for d in range(owners)]
        arrived[0, (0, 0), 1] = lax.ppermute(raw, "snap", pairs)
    for kind, step in schedule_of(bits):
        if kind == "make":
            stage, launch, chosen = step
            sent = send_call(
                flows, chosen, stage, launch, group, me, table, coefficients,
                snapshots, arrived,
            )
            made.update({(stage, *key): value for key, value in sent.items()})
        elif kind == "hold":
            helds[step] = held_call(
                flows[step], step, group, me, table, coefficients, snapshots, arrived
            )
        else:
            stage, _, f = step
            pairs = [(d, d ^ (1 << flows[f][2][stage])) for d in range(owners)]
            arrived[step] = lax.ppermute(made[step], "snap", pairs)
    return last_call(flows, snapshots, [helds[f] for f in range(len(flows))], arrived)


def solution(mesh):
    return jax.shard_map(
        on_device,
        mesh=mesh,
        in_specs=(P("snap", "row", None), P("snap"), P(("snap", "row")), P()),
        out_specs=P(None, "row", "snap"),
        check_vma=False,
    )
```
